32 devices in a mesh: grp: 4 (over y, x), dev: 8 (over z, core).
Axes of the slice: x: 2, y: 2, z: 4, core: 2. Of those that a mesh axis runs over, the one named last changes fastest.
Arguments:
- nz_user: int32 [4096, 128], P(('grp', 'dev')), may hold values from 0 to 8191
- nz_sub: int32 [4096, 128], P(('grp', 'dev')), may hold values from 0 to 2047
- nz_value: float32 [4096, 128], P(('grp', 'dev')), may hold values from -1 to 1
- tile_word: int32 [4096], P(('grp', 'dev')), may hold values from 0 to 2047, as said below
- word_owner: int32 [2048], replicated, may hold values from 0 to 2047, as said below
- user_factor: bfloat16 [64, 8192], P(None, 'dev'), may hold values from -6 to 6
- sub_factor: bfloat16 [64, 2048], P(None, 'dev'), may hold values from -6 to 6
Outputs:
- word_rows: float32 [64, 2048], P(None, ('grp', 'dev'))
The draws below stay inside these ranges and needn't reach their ends.
Inputs may be any that keep to these rules, and one draw needn't show every extreme that they name: A permutation of the word indices: word w is summed into column word_owner[w] of word_rows. `tile_word`: tile i lies on device i // 128 (grp+dev order). On every device at most 2 tiles belong to words whose output column lies on any one other device, and on every device that bound is reached for some other device.
All inputs are finite; a program needn't handle non-finite values.
Results may differ from the reference program's by a relative error of at most 0.0003.
Values may be sent and summed in bfloat16 or wider, within the bound.
A program may use at most 64 MiB of HBM per device.

```python
import math
import jax
import jax.numpy as jnp
import numpy as np
from jax import lax

RANK = 64
NZ = 128
CAP = 2
TILES_DEV = 128
WORDS_DEV = 64
TILES = 4096
USERS = 8192
SUBS = 2048
WORDS = 2048


def layout(key):
    devices_all = TILES // TILES_DEV
    owner_key = jax.random.fold_in(key, 11)
    word_owner = jax.random.permutation(owner_key, WORDS).astype(jnp.int32)
    word_of_row = jnp.zeros((WORDS,), jnp.int32).at[word_owner].set(jnp.arange(WORDS, dtype=jnp.int32))
    heavy_count = min(4, WORDS_DEV)
    heavy_key = jax.random.fold_in(key, 17)

    def heavy_rows(device_index):
        return jax.random.permutation(jax.random.fold_in(heavy_key, device_index), WORDS_DEV)[:heavy_count].astype(jnp.int32)
    heavy_table = jax.vmap(heavy_rows)(jnp.arange(devices_all, dtype=jnp.int32))

    def one_device(device_index):
        device_key = jax.random.fold_in(jax.random.fold_in(key, 23), device_index)
        key_list = jax.random.split(device_key, 6)
        hot_device = (device_index + 1 + jax.random.randint(key_list[0], (), 0, devices_all - 1)) % devices_all
        pair_ids = jnp.arange(devices_all * CAP, dtype=jnp.int32)
        pair_target = pair_ids // CAP
        order_key = jax.random.permutation(key_list[1], devices_all * CAP).astype(jnp.int32)
        order_key = jnp.where(pair_target == hot_device, -1 - pair_ids % CAP, order_key)
        pair_order = pair_target[jnp.argsort(order_key, stable=True)]
        remote_count = jnp.minimum(jax.random.randint(key_list[2], (), 3 * TILES_DEV // 16, 3 * TILES_DEV // 8 + 1), devices_all * CAP)
        slot_ids = jnp.arange(TILES_DEV, dtype=jnp.int32)
        padded_order = pair_order[jnp.minimum(slot_ids, devices_all * CAP - 1)]
        destination = jnp.where(slot_ids < remote_count, padded_order, device_index).astype(jnp.int32)
        heavy_pick = jax.random.randint(key_list[3], (TILES_DEV,), 0, heavy_count)
        light_pick = jax.random.randint(key_list[4], (TILES_DEV,), 0, WORDS_DEV)
        offset = jnp.where(destination == device_index, light_pick, heavy_table[destination, heavy_pick]).astype(jnp.int32)
        words = word_of_row[destination * WORDS_DEV + offset]
        shuffle = jax.random.permutation(key_list[5], TILES_DEV)
        return words[shuffle].astype(jnp.int32)
    tile_word = jax.vmap(one_device)(jnp.arange(devices_all, dtype=jnp.int32)).reshape(TILES)
    return (word_owner, tile_word)


def draw_word_owner(key, part):
    return layout(key)[0]


def draw_tile_word(key, part):
    return layout(key)[1]


def draw_nz_value(key, part):
    key_list = jax.random.split(jax.random.fold_in(key, 37), 3)
    live_count = jax.random.randint(key_list[0], (TILES, 1), NZ // 4, NZ + 1)
    filled = (jnp.arange(NZ)[None, :] < live_count).astype(jnp.float32)
    raw_values = 0.125 * jax.random.normal(key_list[2], (TILES, NZ))
    return (jnp.clip(raw_values, -1.0, 1.0) * filled).astype(jnp.float32)


def place_ends(result, key, least, high):
    place = [jax.random.randint(jax.random.fold_in(key, axis), (), 0, length) for axis, length in enumerate(result.shape)]
    longest = result.shape.index(max(result.shape))
    next_to = place[:longest] + [(place[longest] + 1) % result.shape[longest]] + place[longest + 1:]
    return result.at[tuple(place)].set(least).at[tuple(next_to)].set(high)


def levels(rng, dims, cuts, least, largest):
    def one(dim, blocks):
        draws = jax.random.uniform(jax.random.fold_in(jax.random.fold_in(rng, 6), dim), (blocks,), jnp.float32, least / len(cuts), largest / len(cuts))
        return jnp.repeat(jnp.exp(draws), dims[dim] // blocks).reshape((-1,) + (1,) * (len(dims) - dim - 1))

    factor_of = one(*cuts[0])
    for cut in cuts[1:]:
        factor_of = factor_of * one(*cut)
    return factor_of


def rank_bounds(amount, slope):
    portions = [(1 << 20) // math.isqrt(standing ** slope) + 1 for standing in range(1, amount + 1)]
    deviation = 1 + sum(portions) // (1 << 30)
    return np.cumsum(np.array([max(1, weight // deviation) for weight in portions]))


def skewed_ids(key, dims, number_of, lean):
    listing = rank_bounds(number_of, lean)
    lot = jax.random.randint(jax.random.fold_in(key, 1), dims, 0, int(listing[number_of - 1]))
    rank = jnp.searchsorted(jnp.asarray(listing, jnp.int32), lot, side="right")
    return jax.random.permutation(jax.random.fold_in(key, 2), number_of)[rank].astype(jnp.int32)


def bell_draw(own_key, shape, deviation, limit, cuts=(), held_as=jnp.bfloat16):
    entries = deviation * jax.random.normal(own_key, shape, jnp.float32)
    if cuts:
        entries = entries * levels(own_key, shape, cuts, -0.22, 0.18)
    return jnp.clip(entries, -limit, limit).astype(held_as)


def setup_inputs(seed: int = 0) -> dict:
    seeds = jax.random.split(jax.random.key(seed), 8)
    return {
        "nz_user": place_ends(jax.random.randint(seeds[0], (TILES, NZ), 0, USERS), jax.random.fold_in(seeds[0], 1), 0, USERS - 1).astype(jnp.int32),
        "nz_sub": place_ends(skewed_ids(seeds[1], (TILES, NZ), SUBS, 2), jax.random.fold_in(seeds[1], 3), 0, SUBS - 1).astype(jnp.int32),
        "nz_value": draw_nz_value(jax.random.fold_in(seeds[7], 71), 0),
        "tile_word": draw_tile_word(jax.random.fold_in(seeds[7], 71), 0),
        "word_owner": draw_word_owner(jax.random.fold_in(seeds[7], 71), 0),
        "user_factor": bell_draw(seeds[5], (RANK, USERS), 1.0, 6.0, ((1, 8),)),
        "sub_factor": bell_draw(seeds[6], (RANK, SUBS), 1.0, 6.0, ((1, 8),)),
    }


def reference(nz_user, nz_sub, nz_value, tile_word, word_owner, user_factor, sub_factor):
    tile_total, tile_width = nz_user.shape
    block_tiles = min(tile_total, 256)
    block_count = tile_total // block_tiles

    def one_block(block_args):
        users_block, subs_block, vals_block = block_args
        user_cols = jnp.take(user_factor, users_block, axis=1).astype(jnp.float32)
        sub_cols = jnp.take(sub_factor, subs_block, axis=1).astype(jnp.float32)
        return jnp.sum(user_cols * sub_cols * vals_block[None], axis=2)

    block_sums = lax.map(one_block, (nz_user.reshape(block_count, block_tiles, tile_width),
                                     nz_sub.reshape(block_count, block_tiles, tile_width),
                                     nz_value.reshape(block_count, block_tiles, tile_width)))
    partial_value = jnp.transpose(block_sums, (1, 0, 2)).reshape(block_sums.shape[1], tile_total)
    out_rows = jnp.take(word_owner, tile_word)
    return jnp.zeros((partial_value.shape[0], WORDS), jnp.float32).at[:, out_rows].add(partial_value)
```

```python
import functools
import jax
import jax.numpy as jnp
from jax import lax
from jax.experimental import pallas as pl
from jax.experimental.pallas import tpu as pltpu

CAP = 2
LANES = 128
VMEM = pltpu.VMEM
HIGH = lax.Precision.HIGHEST
MESH = pl.DeviceIdType.MESH


def packed(x):
    half = x.shape[1] // 2
    x = x.astype(jnp.float32)
    return jnp.concatenate([x[:, :half], x[:, half:]], axis=0).T.astype(jnp.bfloat16)


def gather_kernel(n_grp, n_dev, uf_ref, sf_ref, out_ref, send_a, recv_a, send_b, recv_b, send_c, recv_c):
    grp, dev = lax.axis_index("grp"), lax.axis_index("dev")
    pairs = n_dev // 2
    pos, core = dev // 2, lax.rem(dev, 2)
    sibling = dev + 1 - 2 * core
    rows = out_ref.shape[2]
    barrier = pltpu.get_barrier_semaphore()
    order = sorted(range(1, pairs), key=lambda k: min(k, pairs - k))
    others = [((pos + k) % pairs) for k in order]
    groups = [lax.rem(grp + j, n_grp) for j in range(1, n_grp)]
    for p in others:
        pl.semaphore_signal(barrier, inc=1, device_id=(grp, 2 * p + core), device_id_type=MESH)
    for g in groups:
        pl.semaphore_signal(barrier, inc=1, device_id=(g, dev), device_id_type=MESH)
    pl.semaphore_signal(barrier, inc=1, device_id=(grp, sibling), device_id_type=MESH)

    block = jnp.concatenate([packed(uf_ref[...]), packed(sf_ref[...])], axis=0)
    for q in range(n_grp):
        out_ref[q, dev] = block[q * rows:(q + 1) * rows]
    pl.semaphore_wait(barrier, len(others) + len(groups) + 1)

    def copy(q, d, send, recv, to):
        return pltpu.make_async_remote_copy(
            src_ref=out_ref.at[q, d], dst_ref=out_ref.at[q, d], send_sem=send, recv_sem=recv,
            device_id=to, device_id_type=MESH)

    sent = []

    def start(c):
        c.start()
        sent.append(c)

    def to_sibling(q, p):
        start(copy(q, 2 * p + core, send_c.at[q, p], recv_c.at[q, p], (grp, sibling)))

    for p in others:
        start(copy(grp, dev, send_a.at[p], recv_a.at[pos], (grp, 2 * p + core)))
    for q in range(n_grp):
        to_sibling(q, pos)
    for p in others:
        d = 2 * p + core
        copy(grp, d, send_a.at[p], recv_a.at[p], (grp, d)).wait_recv()
        for g in groups:
            start(copy(grp, d, send_b.at[g, p], recv_b.at[grp, p], (g, dev)))
        to_sibling(grp, p)
    for p in others:
        for g in groups:
            d = 2 * p + core
            copy(g, d, send_b.at[g, p], recv_b.at[g, p], (g, dev)).wait_recv()
            to_sibling(g, p)
    for p in [pos] + others:
        for q in range(n_grp):
            copy(q, 2 * p + (1 - core), send_c.at[q, p], recv_c.at[q, p], (grp, sibling)).wait_recv()
    for c in sent:
        c.wait_send()


def gather_tables(n_grp, n_dev, uf, sf):
    rows = (uf.shape[1] + sf.shape[1]) // 2 // n_grp
    pairs = n_dev // 2
    dma = pltpu.SemaphoreType.DMA
    return pl.pallas_call(
        functools.partial(gather_kernel, n_grp, n_dev),
        out_shape=jax.ShapeDtypeStruct((n_grp, n_dev, rows, LANES), jnp.bfloat16),
        in_specs=[pl.BlockSpec(memory_space=VMEM)] * 2,
        out_specs=pl.BlockSpec(memory_space=VMEM),
        scratch_shapes=[dma((pairs,)), dma((pairs,)), dma((n_grp, pairs)), dma((n_grp, pairs)),
                        dma((n_grp, pairs)), dma((n_grp, pairs))],
        compiler_params=pltpu.CompilerParams(collective_id=0, has_side_effects=True),
        name="gather_tables",
    )(uf, sf)


def tile_kernel(user_dev, sub_dev, tab_ref, val_ref, user_hbm, sub_hbm, word_hbm, owner_hbm, out_ref,
                utab, stab, vt, prod, users, subs, words, owners, sems):
    copies = [pltpu.make_async_copy(src, dst, sems.at[i]) for i, (src, dst) in enumerate(
        [(user_hbm, users), (sub_hbm, subs), (word_hbm, words), (owner_hbm, owners)])]
    for c in copies:
        c.start()
    n_grp, n_dev, rows, lanes = tab_ref.shape
    tiles, width = users.shape
    rank = lanes // 2
    user_half, sub_half = user_dev // 2, sub_dev // 2

    def fill(d, carry):
        for q in range(n_grp):
            lo, hi = q * rows, (q + 1) * rows
            for table, first, last, size in ((utab, 0, user_half, user_dev),
                                             (stab, user_half, user_half + sub_half, sub_dev)):
                a, b = max(lo, first), min(hi, last)
                if a >= b:
                    continue
                x = tab_ref[q, d, a - lo:b - lo, :].astype(jnp.float32)
                base = d * size + (a - first)
                table[pl.ds(pl.multiple_of(base, 8), b - a), :] = x
                table[pl.ds(pl.multiple_of(base + size // 2, 8), b - a), :] = pltpu.roll(x, rank, 1)
        return carry

    lax.fori_loop(0, n_dev, fill, 0)
    vt[...] = val_ref[...].T
    for c in copies:
        c.wait()
    lane = lax.broadcasted_iota(jnp.int32, (1, lanes), 1)

    def one_tile(t, carry):
        for n in range(width):
            u, s = users[t, n], subs[t, n]
            prod[n:n + 1, :] = utab[pl.ds(u, 1), :] * stab[pl.ds(s, 1), :]
        vals = pltpu.roll(vt[...], tiles - t, 1)[:, 0:1]
        row = jnp.sum(prod[...] * vals, axis=0, keepdims=True)
        owner = owners[words[t]].astype(jnp.float32)
        out_ref[pl.ds(t, 1), :] = jnp.where(lane < rank, row, owner)
        return carry

    lax.fori_loop(0, tiles, one_tile, 0)


def tile_rows(tables, user_dev, sub_dev, nz_user, nz_sub, nz_value, tile_word, word_owner):
    tiles, width = nz_user.shape
    n_dev = tables.shape[1]
    any_spec = pl.BlockSpec(memory_space=pl.ANY)
    vmem = pl.BlockSpec(memory_space=VMEM)
    return pl.pallas_call(
        functools.partial(tile_kernel, user_dev, sub_dev),
        out_shape=jax.ShapeDtypeStruct((tiles, LANES), jnp.float32),
        in_specs=[vmem, vmem, any_spec, any_spec, any_spec, any_spec],
        out_specs=vmem,
        scratch_shapes=[
            VMEM((user_dev * n_dev, LANES), jnp.float32),
            VMEM((sub_dev * n_dev, LANES), jnp.float32),
            VMEM((width, tiles), jnp.float32),
            VMEM((width, LANES), jnp.float32),
            pltpu.SMEM(nz_user.shape, jnp.int32),
            pltpu.SMEM(nz_sub.shape, jnp.int32),
            pltpu.SMEM(tile_word.shape, jnp.int32),
            pltpu.SMEM(word_owner.shape, jnp.int32),
            pltpu.SemaphoreType.DMA((4,)),
        ],
        compiler_params=pltpu.CompilerParams(vmem_limit_bytes=63_000_000),
        name="tile_rows",
    )(tables, nz_value, nz_user, nz_sub, tile_word, word_owner)


def tdot(a, b):
    return lax.dot_general(a, b, (((0,), (0,)), ((), ())), precision=HIGH,
                           preferred_element_type=jnp.float32)


def exchange_kernel(n_grp, n_dev, cols, rows_ref, out_ref, outbox, inbox, send_sem, recv_sem):
    grp, dev = lax.axis_index("grp"), lax.axis_index("dev")
    n_all = n_grp * n_dev
    me = grp * n_dev + dev
    barrier = pltpu.get_barrier_semaphore()
    peers = [lax.rem(me + k, n_all) for k in range(1, n_all)]

    def where_is(p):
        return (p // n_dev, lax.rem(p, n_dev))

    for p in peers:
        pl.semaphore_signal(barrier, inc=1, device_id=where_is(p), device_id_type=MESH)
    rows = rows_ref[...]
    tiles, lanes = rows.shape
    rank = lanes // 2
    lane = lax.broadcasted_iota(jnp.int32, (tiles, lanes), 1)
    owner_row = jnp.where(lane < rank, pltpu.roll(rows, rank, 1), rows).astype(jnp.int32)
    owner = owner_row // cols
    local = owner_row - owner * cols
    slots = n_all * CAP
    slot = lax.broadcasted_iota(jnp.int32, (tiles, slots), 1)
    own_col = owner_row[:, :1]
    owner_col = jnp.broadcast_to(owner[:, :1], (tiles, slots))
    going = jnp.where((owner_col != me) & (owner_col == slot // CAP), 1.0, 0.0)
    earlier = jnp.where(lax.broadcasted_iota(jnp.int32, (tiles, tiles), 0)
                        > lax.broadcasted_iota(jnp.int32, (tiles, tiles), 1), 1.0, 0.0)
    before = jnp.dot(earlier.astype(jnp.bfloat16), going.astype(jnp.bfloat16),
                     preferred_element_type=jnp.float32)
    table = jnp.where(before == (slot - slot // CAP * CAP).astype(jnp.float32), going, 0.0)
    tagged = jnp.where(lane < rank, rows, (local + 1).astype(jnp.float32))
    box = tdot(table, tagged)
    for p in range(n_all):
        outbox[p] = box[p * CAP:(p + 1) * CAP]
    inbox[me] = jnp.zeros((CAP, lanes), jnp.float32)
    pl.semaphore_wait(barrier, n_all - 1)
    copies = []
    for p in peers:
        c = pltpu.make_async_remote_copy(
            src_ref=outbox.at[p], dst_ref=inbox.at[me], send_sem=send_sem.at[p],
            recv_sem=recv_sem.at[me], device_id=where_is(p), device_id_type=MESH)
        c.start()
        copies.append(c)
    col = lax.broadcasted_iota(jnp.int32, (tiles, lanes), 1)
    mine = jnp.where(owner_row == me * cols + col, 1.0, 0.0)
    own_part = tdot(rows, mine)
    for p in peers:
        pltpu.make_async_remote_copy(
            src_ref=outbox.at[p], dst_ref=inbox.at[p], send_sem=send_sem.at[p],
            recv_sem=recv_sem.at[p], device_id=where_is(p), device_id_type=MESH).wait_recv()
    got = jnp.concatenate([inbox[p] for p in range(n_all)], axis=0)
    glane = lax.broadcasted_iota(jnp.int32, (slots, lanes), 1)
    got_row = jnp.where(glane < rank, pltpu.roll(got, rank, 1), got).astype(jnp.int32)
    far_part = tdot(got, jnp.where(got_row == glane + 1, 1.0, 0.0))
    out_ref[...] = (own_part + far_part)[:rank, :cols]
    for c in copies:
        c.wait_send()


def exchange(n_grp, n_dev, cols, rows):
    n_all = n_grp * n_dev
    rank = rows.shape[1] // 2
    return pl.pallas_call(
        functools.partial(exchange_kernel, n_grp, n_dev, cols),
        out_shape=jax.ShapeDtypeStruct((rank, cols), jnp.float32),
        in_specs=[pl.BlockSpec(memory_space=VMEM)],
        out_specs=pl.BlockSpec(memory_space=VMEM),
        scratch_shapes=[
            VMEM((n_all, CAP, LANES), jnp.float32),
            VMEM((n_all, CAP, LANES), jnp.float32),
            pltpu.SemaphoreType.DMA((n_all,)),
            pltpu.SemaphoreType.DMA((n_all,)),
        ],
        compiler_params=pltpu.CompilerParams(collective_id=1, has_side_effects=True),
        name="exchange",
    )(rows)


def solution(mesh):
    n_grp, n_dev = mesh.shape["grp"], mesh.shape["dev"]

    def shards(nz_user, nz_sub, nz_value, tile_word, word_owner, user_factor, sub_factor):
        tables = gather_tables(n_grp, n_dev, user_factor, sub_factor)
        rows = tile_rows(tables, user_factor.shape[1], sub_factor.shape[1],
                         nz_user, nz_sub, nz_value, tile_word, word_owner)
        return exchange(n_grp, n_dev, word_owner.shape[0] // (n_grp * n_dev), rows)

    return jax.shard_map(
        shards,
        mesh=mesh,
        in_specs=(
            jax.sharding.PartitionSpec(("grp", "dev"), None),
            jax.sharding.PartitionSpec(("grp", "dev"), None),
            jax.sharding.PartitionSpec(("grp", "dev"), None),
            jax.sharding.PartitionSpec(("grp", "dev")),
            jax.sharding.PartitionSpec(),
            jax.sharding.PartitionSpec(None, "dev"),
            jax.sharding.PartitionSpec(None, "dev"),
        ),
        out_specs=jax.sharding.PartitionSpec(None, ("grp", "dev")),
        check_vma=False,
    )
```

```python
import functools
import jax
import jax.numpy as jnp
from jax import lax
from jax.experimental import pallas as pl
from jax.experimental.pallas import tpu as pltpu

CAP = 2
LANES = 128
VMEM = pltpu.VMEM
HIGH = lax.Precision.HIGHEST
MESH = pl.DeviceIdType.MESH


def packed(x):
    half = x.shape[1] // 2
    x = x.astype(jnp.float32)
    return jnp.concatenate([x[:, :half], x[:, half:]], axis=0).T.astype(jnp.bfloat16)


def gather_kernel(n_grp, n_dev, uf_ref, sf_ref, out_ref, send_a, recv_a, send_b, recv_b, send_c, recv_c):
    grp, dev = lax.axis_index("grp"), lax.axis_index("dev")
    pairs = n_dev // 2
    pos, core = dev // 2, lax.rem(dev, 2)
    sibling = dev + 1 - 2 * core
    rows = out_ref.shape[2]
    barrier = pltpu.get_barrier_semaphore()
    order = sorted(range(1, pairs), key=lambda k: min(k, pairs - k))
    others = [((pos + k) % pairs) for k in order]
    groups = [lax.rem(grp + j, n_grp) for j in range(1, n_grp)]
    for p in others:
        pl.semaphore_signal(barrier, inc=1, device_id=(grp, 2 * p + core), device_id_type=MESH)
    for g in groups:
        pl.semaphore_signal(barrier, inc=1, device_id=(g, dev), device_id_type=MESH)
    pl.semaphore_signal(barrier, inc=1, device_id=(grp, sibling), device_id_type=MESH)

    block = jnp.concatenate([packed(uf_ref[...]), packed(sf_ref[...])], axis=0)
    for q in range(n_grp):
        out_ref[q, dev] = block[q * rows:(q + 1) * rows]
    pl.semaphore_wait(barrier, len(others) + len(groups) + 1)

    def copy(q, d, send, recv, to):
        return pltpu.make_async_remote_copy(
            src_ref=out_ref.at[q, d], dst_ref=out_ref.at[q, d], send_sem=send, recv_sem=recv,
            device_id=to, device_id_type=MESH)

    sent = []

    def start(c):
        c.start()
        sent.append(c)

    def to_sibling(q, p):
        start(copy(q, 2 * p + core, send_c.at[q, p], recv_c.at[q, p], (grp, sibling)))

    for p in others:
        start(copy(grp, dev, send_a.at[p], recv_a.at[pos], (grp, 2 * p + core)))
    for q in range(n_grp):
        to_sibling(q, pos)
    for p in others:
        d = 2 * p + core
        copy(grp, d, send_a.at[p], recv_a.at[p], (grp, d)).wait_recv()
        for g in groups:
            start(copy(grp, d, send_b.at[g, p], recv_b.at[grp, p], (g, dev)))
        to_sibling(grp, p)
    for p in others:
        for g in groups:
            d = 2 * p + core
            copy(g, d, send_b.at[g, p], recv_b.at[g, p], (g, dev)).wait_recv()
            to_sibling(g, p)
    for p in [pos] + others:
        for q in range(n_grp):
            copy(q, 2 * p + (1 - core), send_c.at[q, p], recv_c.at[q, p], (grp, sibling)).wait_recv()
    for c in sent:
        c.wait_send()


def gather_tables(n_grp, n_dev, uf, sf):
    rows = (uf.shape[1] + sf.shape[1]) // 2 // n_grp
    pairs = n_dev // 2
    dma = pltpu.SemaphoreType.DMA
    return pl.pallas_call(
        functools.partial(gather_kernel, n_grp, n_dev),
        out_shape=jax.ShapeDtypeStruct((n_grp, n_dev, rows, LANES), jnp.bfloat16),
        in_specs=[pl.BlockSpec(memory_space=VMEM)] * 2,
        out_specs=pl.BlockSpec(memory_space=VMEM),
        scratch_shapes=[dma((pairs,)), dma((pairs,)), dma((n_grp, pairs)), dma((n_grp, pairs)),
                        dma((n_grp, pairs)), dma((n_grp, pairs))],
        compiler_params=pltpu.CompilerParams(collective_id=0, has_side_effects=True),
        name="gather_tables",
    )(uf, sf)


def fill_tables(tab_ref, d, user_dev, sub_dev, utab, stab):
    n_grp, _, rows, lanes = tab_ref.shape
    rank = lanes // 2
    user_half, sub_half = user_dev // 2, sub_dev // 2
    for q in range(n_grp):
        lo, hi = q * rows, (q + 1) * rows
        for table, first, last, size in ((utab, 0, user_half, user_dev),
                                         (stab, user_half, user_half + sub_half, sub_dev)):
            a, b = max(lo, first), min(hi, last)
            if a >= b:
                continue
            x = tab_ref[q, d, a - lo:b - lo, :].astype(jnp.float32)
            base = d * size + (a - first)
            table[pl.ds(pl.multiple_of(base, 8), b - a), :] = x
            table[pl.ds(pl.multiple_of(base + size // 2, 8), b - a), :] = pltpu.roll(x, rank, 1)


STEP = 8


def index_copies(c, half, user_hbm, sub_hbm, users, subs, sems):
    rows = pl.ds(pl.multiple_of(c * STEP, STEP), STEP)
    return [pltpu.make_async_copy(user_hbm.at[rows], users[half], sems.at[half, 0]),
            pltpu.make_async_copy(sub_hbm.at[rows], subs[half], sems.at[half, 1])]


def sum_tiles(user_hbm, sub_hbm, val_ref, words, owners, out_ref, utab, stab, prod, users, subs, sems):
    tiles, lanes = out_ref.shape
    rank = lanes // 2
    width = val_ref.shape[1]
    chunks = tiles // STEP
    lane = lax.broadcasted_iota(jnp.int32, (1, lanes), 1)

    def chunk(c, half):
        for copy in index_copies(c, half, user_hbm, sub_hbm, users, subs, sems):
            copy.wait()
        base = pl.multiple_of(c * STEP, STEP)
        vals = val_ref[pl.ds(base, STEP), :].T
        out = []
        for j in range(STEP):
            for n in range(width):
                u, s = users[half][j, n], subs[half][j, n]
                prod[j % 2, n:n + 1, :] = utab[pl.ds(u, 1), :] * stab[pl.ds(s, 1), :]
            row = jnp.sum(prod[j % 2] * vals[:, j:j + 1], axis=0, keepdims=True)
            owner = owners[words[base + j]].astype(jnp.float32)
            out.append(jnp.where(lane < rank, row, owner))
        out_ref[pl.ds(base, STEP), :] = jnp.concatenate(out, axis=0)

    def two_chunks(i, carry):
        for half in range(2):
            c = 2 * i + half
            chunk(c, half)

            @pl.when(i < chunks // 2 - 1)
            def _():
                for copy in index_copies(c + 2, half, user_hbm, sub_hbm, users, subs, sems):
                    copy.start()
        return carry

    lax.fori_loop(0, chunks // 2, two_chunks, 0)


def tile_kernel(user_dev, sub_dev, tab_ref, val_ref, user_hbm, sub_hbm, word_hbm, owner_hbm, out_ref,
                utab, stab, prod, users_a, users_b, subs_a, subs_b, words, owners, sems, word_sems):
    users, subs = (users_a, users_b), (subs_a, subs_b)
    copies = [pltpu.make_async_copy(word_hbm, words, word_sems.at[0]),
              pltpu.make_async_copy(owner_hbm, owners, word_sems.at[1])]
    for half in range(2):
        for c in index_copies(half, half, user_hbm, sub_hbm, users, subs, sems):
            c.start()
    for c in copies:
        c.start()

    def fill(d, carry):
        fill_tables(tab_ref, d, user_dev, sub_dev, utab, stab)
        return carry

    lax.fori_loop(0, tab_ref.shape[1], fill, 0)
    for c in copies:
        c.wait()
    sum_tiles(user_hbm, sub_hbm, val_ref, words, owners, out_ref, utab, stab, prod, users, subs, sems)


def tile_rows(tables, user_dev, sub_dev, nz_user, nz_sub, nz_value, tile_word, word_owner):
    tiles, width = nz_user.shape
    n_dev = tables.shape[1]
    any_spec = pl.BlockSpec(memory_space=pl.ANY)
    vmem = pl.BlockSpec(memory_space=VMEM)
    return pl.pallas_call(
        functools.partial(tile_kernel, user_dev, sub_dev),
        out_shape=jax.ShapeDtypeStruct((tiles, LANES), jnp.float32),
        in_specs=[vmem, vmem, any_spec, any_spec, any_spec, any_spec],
        out_specs=vmem,
        scratch_shapes=[
            VMEM((user_dev * n_dev, LANES), jnp.float32),
            VMEM((sub_dev * n_dev, LANES), jnp.float32),
            VMEM((2, width, LANES), jnp.float32),
            pltpu.SMEM((STEP, width), jnp.int32),
            pltpu.SMEM((STEP, width), jnp.int32),
            pltpu.SMEM((STEP, width), jnp.int32),
            pltpu.SMEM((STEP, width), jnp.int32),
            pltpu.SMEM(tile_word.shape, jnp.int32),
            pltpu.SMEM(word_owner.shape, jnp.int32),
            pltpu.SemaphoreType.DMA((2, 2)),
            pltpu.SemaphoreType.DMA((2,)),
        ],
        compiler_params=pltpu.CompilerParams(vmem_limit_bytes=63_000_000),
        name="tile_rows",
    )(tables, nz_value, nz_user, nz_sub, tile_word, word_owner)


def tdot(a, b):
    return lax.dot_general(a, b, (((0,), (0,)), ((), ())), precision=HIGH,
                           preferred_element_type=jnp.float32)


def exchange_kernel(n_grp, n_dev, cols, rows_ref, out_ref, outbox, inbox, send_sem, recv_sem):
    grp, dev = lax.axis_index("grp"), lax.axis_index("dev")
    n_all = n_grp * n_dev
    me = grp * n_dev + dev
    barrier = pltpu.get_barrier_semaphore()
    peers = [lax.rem(me + k, n_all) for k in range(1, n_all)]

    def where_is(p):
        return (p // n_dev, lax.rem(p, n_dev))

    for p in peers:
        pl.semaphore_signal(barrier, inc=1, device_id=where_is(p), device_id_type=MESH)
    rows = rows_ref[...]
    tiles, lanes = rows.shape
    rank = lanes // 2
    lane = lax.broadcasted_iota(jnp.int32, (tiles, lanes), 1)
    owner_row = jnp.where(lane < rank, pltpu.roll(rows, rank, 1), rows).astype(jnp.int32)
    owner = owner_row // cols
    local = owner_row - owner * cols
    slots = n_all * CAP
    slot = lax.broadcasted_iota(jnp.int32, (tiles, slots), 1)
    own_col = owner_row[:, :1]
    owner_col = jnp.broadcast_to(owner[:, :1], (tiles, slots))
    going = jnp.where((owner_col != me) & (owner_col == slot // CAP), 1.0, 0.0)
    earlier = jnp.where(lax.broadcasted_iota(jnp.int32, (tiles, tiles), 0)
                        > lax.broadcasted_iota(jnp.int32, (tiles, tiles), 1), 1.0, 0.0)
    before = jnp.dot(earlier.astype(jnp.bfloat16), going.astype(jnp.bfloat16),
                     preferred_element_type=jnp.float32)
    table = jnp.where(before == (slot - slot // CAP * CAP).astype(jnp.float32), going, 0.0)
    tagged = jnp.where(lane < rank, rows, (local + 1).astype(jnp.float32))
    box = tdot(table, tagged)
    for p in range(n_all):
        outbox[p] = box[p * CAP:(p + 1) * CAP]
    inbox[me] = jnp.zeros((CAP, lanes), jnp.float32)
    pl.semaphore_wait(barrier, n_all - 1)
    copies = []
    for p in peers:
        c = pltpu.make_async_remote_copy(
            src_ref=outbox.at[p], dst_ref=inbox.at[me], send_sem=send_sem.at[p],
            recv_sem=recv_sem.at[me], device_id=where_is(p), device_id_type=MESH)
        c.start()
        copies.append(c)
    col = lax.broadcasted_iota(jnp.int32, (tiles, lanes), 1)
    mine = jnp.where(owner_row == me * cols + col, 1.0, 0.0)
    own_part = tdot(rows, mine)
    for p in peers:
        pltpu.make_async_remote_copy(
            src_ref=outbox.at[p], dst_ref=inbox.at[p], send_sem=send_sem.at[p],
            recv_sem=recv_sem.at[p], device_id=where_is(p), device_id_type=MESH).wait_recv()
    got = jnp.concatenate([inbox[p] for p in range(n_all)], axis=0)
    glane = lax.broadcasted_iota(jnp.int32, (slots, lanes), 1)
    got_row = jnp.where(glane < rank, pltpu.roll(got, rank, 1), got).astype(jnp.int32)
    far_part = tdot(got, jnp.where(got_row == glane + 1, 1.0, 0.0))
    out_ref[...] = (own_part + far_part)[:rank, :cols]
    for c in copies:
        c.wait_send()


def exchange(n_grp, n_dev, cols, rows):
    n_all = n_grp * n_dev
    rank = rows.shape[1] // 2
    return pl.pallas_call(
        functools.partial(exchange_kernel, n_grp, n_dev, cols),
        out_shape=jax.ShapeDtypeStruct((rank, cols), jnp.float32),
        in_specs=[pl.BlockSpec(memory_space=VMEM)],
        out_specs=pl.BlockSpec(memory_space=VMEM),
        scratch_shapes=[
            VMEM((n_all, CAP, LANES), jnp.float32),
            VMEM((n_all, CAP, LANES), jnp.float32),
            pltpu.SemaphoreType.DMA((n_all,)),
            pltpu.SemaphoreType.DMA((n_all,)),
        ],
        compiler_params=pltpu.CompilerParams(collective_id=1, has_side_effects=True),
        name="exchange",
    )(rows)


def solution(mesh):
    n_grp, n_dev = mesh.shape["grp"], mesh.shape["dev"]

    def shards(nz_user, nz_sub, nz_value, tile_word, word_owner, user_factor, sub_factor):
        tables = gather_tables(n_grp, n_dev, user_factor, sub_factor)
        rows = tile_rows(tables, user_factor.shape[1], sub_factor.shape[1],
                         nz_user, nz_sub, nz_value, tile_word, word_owner)
        return exchange(n_grp, n_dev, word_owner.shape[0] // (n_grp * n_dev), rows)

    return jax.shard_map(
        shards,
        mesh=mesh,
        in_specs=(
            jax.sharding.PartitionSpec(("grp", "dev"), None),
            jax.sharding.PartitionSpec(("grp", "dev"), None),
            jax.sharding.PartitionSpec(("grp", "dev"), None),
            jax.sharding.PartitionSpec(("grp", "dev")),
            jax.sharding.PartitionSpec(),
            jax.sharding.PartitionSpec(None, "dev"),
            jax.sharding.PartitionSpec(None, "dev"),
        ),
        out_specs=jax.sharding.PartitionSpec(None, ("grp", "dev")),
        check_vma=False,
    )
```

```python
import functools
import jax
import jax.numpy as jnp
from jax import lax
from jax.experimental import pallas as pl
from jax.experimental.pallas import tpu as pltpu

CAP = 2
LANES = 128
VMEM = pltpu.VMEM
HIGH = lax.Precision.HIGHEST
MESH = pl.DeviceIdType.MESH


def packed(x):
    half = x.shape[1] // 2
    x = x.astype(jnp.float32)
    return jnp.concatenate([x[:, :half], x[:, half:]], axis=0).T.astype(jnp.bfloat16)


def where_is(n_dev, p):
    return (p // n_dev, lax.rem(p, n_dev))


def gather_tables(n_grp, n_dev, uf_ref, sf_ref, tab, arrived, barrier_wait,
                  send_a, recv_a, send_b, recv_b, send_c, recv_c):
    grp, dev = lax.axis_index("grp"), lax.axis_index("dev")
    pairs = n_dev // 2
    pos, core = dev // 2, lax.rem(dev, 2)
    sibling = dev + 1 - 2 * core
    rows = tab.shape[2]
    order = sorted(range(1, pairs), key=lambda k: min(k, pairs - k))
    others = [((pos + k) % pairs) for k in order]
    groups = [lax.rem(grp + j, n_grp) for j in range(1, n_grp)]
    block = jnp.concatenate([packed(uf_ref[...]), packed(sf_ref[...])], axis=0)
    for q in range(n_grp):
        tab[q, dev] = block[q * rows:(q + 1) * rows]
    barrier_wait()

    def copy(q, d, send, recv, to):
        return pltpu.make_async_remote_copy(
            src_ref=tab.at[q, d], dst_ref=tab.at[q, d], send_sem=send, recv_sem=recv,
            device_id=to, device_id_type=MESH)

    sent = []

    def start(c):
        c.start()
        sent.append(c)

    def to_sibling(q, p):
        start(copy(q, 2 * p + core, send_c.at[q, p], recv_c.at[q, p], (grp, sibling)))

    for p in others:
        start(copy(grp, dev, send_a.at[p], recv_a.at[pos], (grp, 2 * p + core)))
    for q in range(n_grp):
        to_sibling(q, pos)
    arrived(dev)
    for p in others:
        d = 2 * p + core
        copy(grp, d, send_a.at[p], recv_a.at[p], (grp, d)).wait_recv()
        for g in groups:
            start(copy(grp, d, send_b.at[g, p], recv_b.at[grp, p], (g, dev)))
        to_sibling(grp, p)
    for q in range(n_grp):
        copy(q, sibling, send_c.at[q, pos], recv_c.at[q, pos], (grp, sibling)).wait_recv()
    arrived(sibling)
    for p in others:
        d = 2 * p + core
        for g in groups:
            copy(g, d, send_b.at[g, p], recv_b.at[g, p], (g, dev)).wait_recv()
            to_sibling(g, p)
        arrived(d)
    for p in others:
        d = 2 * p + (1 - core)
        for q in range(n_grp):
            copy(q, d, send_c.at[q, p], recv_c.at[q, p], (grp, sibling)).wait_recv()
        arrived(d)
    return sent


def fill_tables(tab_ref, d, user_dev, sub_dev, utab, stab):
    n_grp, _, rows, lanes = tab_ref.shape
    rank = lanes // 2
    user_half, sub_half = user_dev // 2, sub_dev // 2
    for q in range(n_grp):
        lo, hi = q * rows, (q + 1) * rows
        for table, first, last, size in ((utab, 0, user_half, user_dev),
                                         (stab, user_half, user_half + sub_half, sub_dev)):
            a, b = max(lo, first), min(hi, last)
            if a >= b:
                continue
            x = tab_ref[q, d, a - lo:b - lo, :].astype(jnp.float32)
            base = d * size + (a - first)
            table[pl.ds(pl.multiple_of(base, 8), b - a), :] = x
            table[pl.ds(pl.multiple_of(base + size // 2, 8), b - a), :] = pltpu.roll(x, rank, 1)


STEP = 8


def index_copies(c, half, user_hbm, sub_hbm, users, subs, sems):
    rows = pl.ds(pl.multiple_of(c * STEP, STEP), STEP)
    return [pltpu.make_async_copy(user_hbm.at[rows], users[half], sems.at[half, 0]),
            pltpu.make_async_copy(sub_hbm.at[rows], subs[half], sems.at[half, 1])]


def sum_tiles(user_hbm, sub_hbm, val_ref, words, owners, out_ref, utab, stab, prod, users, subs, sems):
    tiles, lanes = out_ref.shape
    rank = lanes // 2
    width = val_ref.shape[1]
    chunks = tiles // STEP
    lane = lax.broadcasted_iota(jnp.int32, (1, lanes), 1)

    def chunk(c, half):
        for copy in index_copies(c, half, user_hbm, sub_hbm, users, subs, sems):
            copy.wait()
        base = pl.multiple_of(c * STEP, STEP)
        vals = val_ref[pl.ds(base, STEP), :].T
        out = []
        for j in range(STEP):
            for n in range(width):
                u, s = users[half][j, n], subs[half][j, n]
                prod[j % 2, n:n + 1, :] = utab[pl.ds(u, 1), :] * stab[pl.ds(s, 1), :]
            row = jnp.sum(prod[j % 2] * vals[:, j:j + 1], axis=0, keepdims=True)
            owner = owners[words[base + j]].astype(jnp.float32)
            out.append(jnp.where(lane < rank, row, owner))
        out_ref[pl.ds(base, STEP), :] = jnp.concatenate(out, axis=0)

    def two_chunks(i, carry):
        for half in range(2):
            c = 2 * i + half
            chunk(c, half)

            @pl.when(i < chunks // 2 - 1)
            def _():
                for copy in index_copies(c + 2, half, user_hbm, sub_hbm, users, subs, sems):
                    copy.start()
        return carry

    lax.fori_loop(0, chunks // 2, two_chunks, 0)


def tdot(a, b):
    return lax.dot_general(a, b, (((0,), (0,)), ((), ())), precision=HIGH,
                           preferred_element_type=jnp.float32)


def exchange(n_grp, n_dev, cols, rows_ref, out_ref, outbox, inbox, send_sem, recv_sem):
    n_all = n_grp * n_dev
    me = lax.axis_index("grp") * n_dev + lax.axis_index("dev")
    peers = [lax.rem(me + k, n_all) for k in range(1, n_all)]
    rows = rows_ref[...]
    tiles, lanes = rows.shape
    rank = lanes // 2
    lane = lax.broadcasted_iota(jnp.int32, (tiles, lanes), 1)
    owner_row = jnp.where(lane < rank, pltpu.roll(rows, rank, 1), rows).astype(jnp.int32)
    owner = owner_row // cols
    local = owner_row - owner * cols
    slots = n_all * CAP
    slot = lax.broadcasted_iota(jnp.int32, (tiles, slots), 1)
    own_col = owner_row[:, :1]
    owner_col = jnp.broadcast_to(owner[:, :1], (tiles, slots))
    going = jnp.where((owner_col != me) & (owner_col == slot // CAP), 1.0, 0.0)
    earlier = jnp.where(lax.broadcasted_iota(jnp.int32, (tiles, tiles), 0)
                        > lax.broadcasted_iota(jnp.int32, (tiles, tiles), 1), 1.0, 0.0)
    before = jnp.dot(earlier.astype(jnp.bfloat16), going.astype(jnp.bfloat16),
                     preferred_element_type=jnp.float32)
    table = jnp.where(before == (slot - slot // CAP * CAP).astype(jnp.float32), going, 0.0)
    tagged = jnp.where(lane < rank, rows, (local + 1).astype(jnp.float32))
    box = tdot(table, tagged)
    for p in range(n_all):
        outbox[p] = box[p * CAP:(p + 1) * CAP]
    inbox[me] = jnp.zeros((CAP, lanes), jnp.float32)
    copies = []
    for p in peers:
        c = pltpu.make_async_remote_copy(
            src_ref=outbox.at[p], dst_ref=inbox.at[me], send_sem=send_sem.at[p],
            recv_sem=recv_sem.at[me], device_id=where_is(n_dev, p), device_id_type=MESH)
        c.start()
        copies.append(c)
    col = lax.broadcasted_iota(jnp.int32, (tiles, lanes), 1)
    mine = jnp.where(owner_row == me * cols + col, 1.0, 0.0)
    own_part = tdot(rows, mine)
    for p in peers:
        pltpu.make_async_remote_copy(
            src_ref=outbox.at[p], dst_ref=inbox.at[p], send_sem=send_sem.at[p],
            recv_sem=recv_sem.at[p], device_id=where_is(n_dev, p), device_id_type=MESH).wait_recv()
    got = jnp.concatenate([inbox[p] for p in range(n_all)], axis=0)
    glane = lax.broadcasted_iota(jnp.int32, (slots, lanes), 1)
    got_row = jnp.where(glane < rank, pltpu.roll(got, rank, 1), got).astype(jnp.int32)
    far_part = tdot(got, jnp.where(got_row == glane + 1, 1.0, 0.0))
    out_ref[...] = (own_part + far_part)[:rank, :cols]
    for c in copies:
        c.wait_send()


def kernel(n_grp, n_dev, cols, uf_ref, sf_ref, val_ref, user_hbm, sub_hbm, word_hbm, owner_hbm, out_ref,
           tab, utab, stab, prod, users_a, users_b, subs_a, subs_b, words, owners, tile_sums, outbox, inbox,
           sems, word_sems, send_a, recv_a, send_b, recv_b, send_c, recv_c, send_x, recv_x):
    n_all = n_grp * n_dev
    me = lax.axis_index("grp") * n_dev + lax.axis_index("dev")
    barrier = pltpu.get_barrier_semaphore()
    for k in range(1, n_all):
        pl.semaphore_signal(barrier, inc=1, device_id=where_is(n_dev, lax.rem(me + k, n_all)),
                            device_id_type=MESH)
    users, subs = (users_a, users_b), (subs_a, subs_b)
    copies = [pltpu.make_async_copy(word_hbm, words, word_sems.at[0]),
              pltpu.make_async_copy(owner_hbm, owners, word_sems.at[1])]
    for half in range(2):
        for c in index_copies(half, half, user_hbm, sub_hbm, users, subs, sems):
            c.start()
    for c in copies:
        c.start()

    def arrived(d):
        fill_tables(tab, d, uf_ref.shape[1], sf_ref.shape[1], utab, stab)

    sent = gather_tables(n_grp, n_dev, uf_ref, sf_ref, tab, arrived,
                         lambda: pl.semaphore_wait(barrier, n_all - 1),
                         send_a, recv_a, send_b, recv_b, send_c, recv_c)
    for c in copies:
        c.wait()
    sum_tiles(user_hbm, sub_hbm, val_ref, words, owners, tile_sums, utab, stab, prod, users, subs, sems)
    exchange(n_grp, n_dev, cols, tile_sums, out_ref, outbox, inbox, send_x, recv_x)
    for c in sent:
        c.wait_send()


def mttkrp(n_grp, n_dev, nz_user, nz_sub, nz_value, tile_word, word_owner, uf, sf):
    n_all, pairs = n_grp * n_dev, n_dev // 2
    tiles, width = nz_user.shape
    rank, user_dev = uf.shape
    sub_dev = sf.shape[1]
    cols = word_owner.shape[0] // n_all
    rows = (user_dev + sub_dev) // 2 // n_grp
    any_spec = pl.BlockSpec(memory_space=pl.ANY)
    vmem = pl.BlockSpec(memory_space=VMEM)
    dma = pltpu.SemaphoreType.DMA
    return pl.pallas_call(
        functools.partial(kernel, n_grp, n_dev, cols),
        out_shape=jax.ShapeDtypeStruct((rank, cols), jnp.float32),
        in_specs=[vmem, vmem, vmem, any_spec, any_spec, any_spec, any_spec],
        out_specs=vmem,
        scratch_shapes=[
            VMEM((n_grp, n_dev, rows, LANES), jnp.bfloat16),
            VMEM((user_dev * n_dev, LANES), jnp.float32),
            VMEM((sub_dev * n_dev, LANES), jnp.float32),
            VMEM((2, width, LANES), jnp.float32),
            pltpu.SMEM((STEP, width), jnp.int32),
            pltpu.SMEM((STEP, width), jnp.int32),
            pltpu.SMEM((STEP, width), jnp.int32),
            pltpu.SMEM((STEP, width), jnp.int32),
            pltpu.SMEM(tile_word.shape, jnp.int32),
            pltpu.SMEM(word_owner.shape, jnp.int32),
            VMEM((tiles, LANES), jnp.float32),
            VMEM((n_all, CAP, LANES), jnp.float32),
            VMEM((n_all, CAP, LANES), jnp.float32),
            dma((2, 2)), dma((2,)), dma((pairs,)), dma((pairs,)), dma((n_grp, pairs)), dma((n_grp, pairs)),
            dma((n_grp, pairs)), dma((n_grp, pairs)), dma((n_all,)), dma((n_all,)),
        ],
        compiler_params=pltpu.CompilerParams(collective_id=0, has_side_effects=True,
                                             vmem_limit_bytes=63_000_000),
        name="mttkrp",
    )(uf, sf, nz_value, nz_user, nz_sub, tile_word, word_owner)


def solution(mesh):
    n_grp, n_dev = mesh.shape["grp"], mesh.shape["dev"]

    def shards(nz_user, nz_sub, nz_value, tile_word, word_owner, user_factor, sub_factor):
        return mttkrp(n_grp, n_dev, nz_user, nz_sub, nz_value, tile_word, word_owner,
                      user_factor, sub_factor)

    return jax.shard_map(
        shards,
        mesh=mesh,
        in_specs=(
            jax.sharding.PartitionSpec(("grp", "dev"), None),
            jax.sharding.PartitionSpec(("grp", "dev"), None),
            jax.sharding.PartitionSpec(("grp", "dev"), None),
            jax.sharding.PartitionSpec(("grp", "dev")),
            jax.sharding.PartitionSpec(),
            jax.sharding.PartitionSpec(None, "dev"),
            jax.sharding.PartitionSpec(None, "dev"),
        ),
        out_specs=jax.sharding.PartitionSpec(None, ("grp", "dev")),
        check_vma=False,
    )
```

```python
import functools
import jax
import jax.numpy as jnp
from jax import lax
from jax.experimental import pallas as pl
from jax.experimental.pallas import tpu as pltpu

CAP = 2
LANES = 128
VMEM = pltpu.VMEM
HIGH = lax.Precision.HIGHEST
MESH = pl.DeviceIdType.MESH


def packed(x):
    half = x.shape[1] // 2
    x = x.astype(jnp.float32)
    return jnp.concatenate([x[:, :half], x[:, half:]], axis=0).T.astype(jnp.bfloat16)


def where_is(n_dev, p):
    return (p // n_dev, lax.rem(p, n_dev))


def gather_tables(n_grp, n_dev, uf_ref, sf_ref, tab, arrived, barrier_wait,
                  send_a, recv_a, send_b, recv_b, send_c, recv_c):
    grp, dev = lax.axis_index("grp"), lax.axis_index("dev")
    pairs = n_dev // 2
    pos, core = dev // 2, lax.rem(dev, 2)
    sibling = dev + 1 - 2 * core
    rows = tab.shape[2]
    order = sorted(range(1, pairs), key=lambda k: min(k, pairs - k))
    others = [((pos + k) % pairs) for k in order]
    groups = [lax.rem(grp + j, n_grp) for j in range(1, n_grp)]
    block = jnp.concatenate([packed(uf_ref[...]), packed(sf_ref[...])], axis=0)
    for q in range(n_grp):
        tab[q, dev] = block[q * rows:(q + 1) * rows]
    barrier_wait()

    def copy(q, d, send, recv, to):
        return pltpu.make_async_remote_copy(
            src_ref=tab.at[q, d], dst_ref=tab.at[q, d], send_sem=send, recv_sem=recv,
            device_id=to, device_id_type=MESH)

    sent = []

    def start(c):
        c.start()
        sent.append(c)

    def to_sibling(q, p):
        start(copy(q, 2 * p + core, send_c.at[q, p], recv_c.at[q, p], (grp, sibling)))

    for p in others:
        start(copy(grp, dev, send_a.at[p], recv_a.at[pos], (grp, 2 * p + core)))
    for q in range(n_grp):
        to_sibling(q, pos)
    arrived(dev)
    for p in others:
        d = 2 * p + core
        copy(grp, d, send_a.at[p], recv_a.at[p], (grp, d)).wait_recv()
        for g in groups:
            start(copy(grp, d, send_b.at[g, p], recv_b.at[grp, p], (g, dev)))
        to_sibling(grp, p)
    for q in range(n_grp):
        copy(q, sibling, send_c.at[q, pos], recv_c.at[q, pos], (grp, sibling)).wait_recv()
    arrived(sibling)
    for p in others:
        d = 2 * p + core
        for g in groups:
            copy(g, d, send_b.at[g, p], recv_b.at[g, p], (g, dev)).wait_recv()
            to_sibling(g, p)
        arrived(d)
    for p in others:
        d = 2 * p + (1 - core)
        for q in range(n_grp):
            copy(q, d, send_c.at[q, p], recv_c.at[q, p], (grp, sibling)).wait_recv()
        arrived(d)
    return sent


def pieces(n_grp, rows, first, last):
    for q in range(n_grp):
        a, b = max(q * rows, first), min((q + 1) * rows, last)
        if a < b:
            yield q, a, b


def fill_users(tab, d, user_dev, utab):
    n_grp, _, rows, lanes = tab.shape
    half = user_dev // 2
    for q, a, b in pieces(n_grp, rows, 0, half):
        x = tab[q, d, a - q * rows:b - q * rows, :].astype(jnp.float32)
        y = pltpu.roll(x, lanes // 2, 1)
        left = lax.broadcasted_iota(jnp.int32, x.shape, 1) < lanes // 2
        base = d * user_dev + a
        utab[pl.ds(pl.multiple_of(base, 8), b - a), :] = jnp.where(left, x, y)
        utab[pl.ds(pl.multiple_of(base + half, 8), b - a), :] = jnp.where(left, y, x)


def fill_subs(tab, user_dev, sub_dev, stab):
    n_grp, n_dev, rows, lanes = tab.shape
    start, half = user_dev // 2, sub_dev // 2
    for q, a, b in pieces(n_grp, rows, start, start + half):
        for p in range(n_dev // 2):
            even, odd = [tab[q, 2 * p + i, a - q * rows:b - q * rows, :].astype(jnp.float32) for i in range(2)]
            left = lax.broadcasted_iota(jnp.int32, even.shape, 1) < lanes // 2
            at = pl.ds(p * lanes, lanes)
            low = jnp.where(left, even, pltpu.roll(odd, lanes // 2, 1))
            high = jnp.where(left, pltpu.roll(even, lanes // 2, 1), odd)
            stab[a - start:b - start, at] = low.astype(jnp.bfloat16)
            stab[half + a - start:half + b - start, at] = high.astype(jnp.bfloat16)


STEP = 8


def index_copies(c, half, user_hbm, users, sems):
    rows = pl.ds(pl.multiple_of(c * STEP, STEP), STEP)
    return [pltpu.make_async_copy(user_hbm.at[rows], users[half], sems.at[half])]


def sum_tiles(user_hbm, sub_ref, val_ref, words, owners, out_ref, utab, stab, picked, users, sems):
    tiles, lanes = out_ref.shape
    rank = lanes // 2
    width = val_ref.shape[1]
    chunks = tiles // STEP
    depth, wide = stab.shape
    lane = lax.broadcasted_iota(jnp.int32, (1, lanes), 1)
    lanes_of = lax.broadcasted_iota(jnp.int32, (width, lanes), 1)
    side = jnp.where(lanes_of < rank, 0, 1)
    keys = lax.broadcasted_iota(jnp.int32, (width, depth), 1)

    def chunk(c, half):
        for copy in index_copies(c, half, user_hbm, users, sems):
            copy.wait()
        base = pl.multiple_of(c * STEP, STEP)
        vals = val_ref[pl.ds(base, STEP), :].T
        subs = sub_ref[pl.ds(base, STEP), :]
        group = subs // depth
        key = (subs - group * depth).astype(jnp.float32).T.astype(jnp.int32)
        group = group.astype(jnp.float32).T.astype(jnp.int32)
        out = []
        for j in range(STEP):
            for n in range(width):
                picked[j % 2, n:n + 1, :] = utab[pl.ds(users[half][j, n], 1), :]
            onehot = jnp.where(key[:, j:j + 1] == keys, 1.0, 0.0).astype(jnp.bfloat16)
            found = jnp.dot(onehot, stab[...], preferred_element_type=jnp.float32)
            pick = jnp.broadcast_to(group[:, j:j + 1], (width, lanes)) - side
            sub_rows = jnp.where(pick == 0, found[:, :lanes], 0.0)
            for p in range(1, wide // lanes):
                sub_rows = jnp.where(pick == 2 * p, found[:, p * lanes:(p + 1) * lanes], sub_rows)
            row = jnp.sum(picked[j % 2] * sub_rows * vals[:, j:j + 1], axis=0, keepdims=True)
            row = row + pltpu.roll(row, rank, 1)
            owner = owners[words[base + j]].astype(jnp.float32)
            out.append(jnp.where(lane < rank, row, owner))
        out_ref[pl.ds(base, STEP), :] = jnp.concatenate(out, axis=0)

    def two_chunks(i, carry):
        for half in range(2):
            c = 2 * i + half
            chunk(c, half)

            @pl.when(i < chunks // 2 - 1)
            def _():
                for copy in index_copies(c + 2, half, user_hbm, users, sems):
                    copy.start()
        return carry

    lax.fori_loop(0, chunks // 2, two_chunks, 0)


def tdot(a, b):
    return lax.dot_general(a, b, (((0,), (0,)), ((), ())), precision=HIGH,
                           preferred_element_type=jnp.float32)


def exchange(n_grp, n_dev, cols, rows_ref, out_ref, outbox, inbox, send_sem, recv_sem):
    n_all = n_grp * n_dev
    me = lax.axis_index("grp") * n_dev + lax.axis_index("dev")
    peers = [lax.rem(me + k, n_all) for k in range(1, n_all)]
    rows = rows_ref[...]
    tiles, lanes = rows.shape
    rank = lanes // 2
    lane = lax.broadcasted_iota(jnp.int32, (tiles, lanes), 1)
    owner_row = jnp.where(lane < rank, pltpu.roll(rows, rank, 1), rows).astype(jnp.int32)
    owner = owner_row // cols
    local = owner_row - owner * cols
    slots = n_all * CAP
    slot = lax.broadcasted_iota(jnp.int32, (tiles, slots), 1)
    own_col = owner_row[:, :1]
    owner_col = jnp.broadcast_to(owner[:, :1], (tiles, slots))
    going = jnp.where((owner_col != me) & (owner_col == slot // CAP), 1.0, 0.0)
    earlier = jnp.where(lax.broadcasted_iota(jnp.int32, (tiles, tiles), 0)
                        > lax.broadcasted_iota(jnp.int32, (tiles, tiles), 1), 1.0, 0.0)
    before = jnp.dot(earlier.astype(jnp.bfloat16), going.astype(jnp.bfloat16),
                     preferred_element_type=jnp.float32)
    table = jnp.where(before == (slot - slot // CAP * CAP).astype(jnp.float32), going, 0.0)
    tagged = jnp.where(lane < rank, rows, (local + 1).astype(jnp.float32))
    box = tdot(table, tagged)
    for p in range(n_all):
        outbox[p] = box[p * CAP:(p + 1) * CAP]
    inbox[me] = jnp.zeros((CAP, lanes), jnp.float32)
    copies = []
    for p in peers:
        c = pltpu.make_async_remote_copy(
            src_ref=outbox.at[p], dst_ref=inbox.at[me], send_sem=send_sem.at[p],
            recv_sem=recv_sem.at[me], device_id=where_is(n_dev, p), device_id_type=MESH)
        c.start()
        copies.append(c)
    col = lax.broadcasted_iota(jnp.int32, (tiles, lanes), 1)
    mine = jnp.where(owner_row == me * cols + col, 1.0, 0.0)
    own_part = tdot(rows, mine)
    for p in peers:
        pltpu.make_async_remote_copy(
            src_ref=outbox.at[p], dst_ref=inbox.at[p], send_sem=send_sem.at[p],
            recv_sem=recv_sem.at[p], device_id=where_is(n_dev, p), device_id_type=MESH).wait_recv()
    got = jnp.concatenate([inbox[p] for p in range(n_all)], axis=0)
    glane = lax.broadcasted_iota(jnp.int32, (slots, lanes), 1)
    got_row = jnp.where(glane < rank, pltpu.roll(got, rank, 1), got).astype(jnp.int32)
    far_part = tdot(got, jnp.where(got_row == glane + 1, 1.0, 0.0))
    out_ref[...] = (own_part + far_part)[:rank, :cols]
    for c in copies:
        c.wait_send()


def kernel(n_grp, n_dev, cols, uf_ref, sf_ref, val_ref, sub_ref, user_hbm, word_hbm, owner_hbm, out_ref,
           tab, utab, stab, prod, users_a, users_b, words, owners, tile_sums, outbox, inbox,
           sems, word_sems, send_a, recv_a, send_b, recv_b, send_c, recv_c, send_x, recv_x):
    n_all = n_grp * n_dev
    me = lax.axis_index("grp") * n_dev + lax.axis_index("dev")
    barrier = pltpu.get_barrier_semaphore()
    for k in range(1, n_all):
        pl.semaphore_signal(barrier, inc=1, device_id=where_is(n_dev, lax.rem(me + k, n_all)),
                            device_id_type=MESH)
    users = (users_a, users_b)
    copies = [pltpu.make_async_copy(word_hbm, words, word_sems.at[0]),
              pltpu.make_async_copy(owner_hbm, owners, word_sems.at[1])]
    for half in range(2):
        for c in index_copies(half, half, user_hbm, users, sems):
            c.start()
    for c in copies:
        c.start()

    def arrived(d):
        fill_users(tab, d, uf_ref.shape[1], utab)

    sent = gather_tables(n_grp, n_dev, uf_ref, sf_ref, tab, arrived,
                         lambda: pl.semaphore_wait(barrier, n_all - 1),
                         send_a, recv_a, send_b, recv_b, send_c, recv_c)
    for c in copies:
        c.wait()
    fill_subs(tab, uf_ref.shape[1], sf_ref.shape[1], stab)
    sum_tiles(user_hbm, sub_ref, val_ref, words, owners, tile_sums, utab, stab, prod, users, sems)
    exchange(n_grp, n_dev, cols, tile_sums, out_ref, outbox, inbox, send_x, recv_x)
    for c in sent:
        c.wait_send()


def mttkrp(n_grp, n_dev, nz_user, nz_sub, nz_value, tile_word, word_owner, uf, sf):
    n_all, pairs = n_grp * n_dev, n_dev // 2
    tiles, width = nz_user.shape
    rank, user_dev = uf.shape
    sub_dev = sf.shape[1]
    cols = word_owner.shape[0] // n_all
    rows = (user_dev + sub_dev) // 2 // n_grp
    any_spec = pl.BlockSpec(memory_space=pl.ANY)
    vmem = pl.BlockSpec(memory_space=VMEM)
    dma = pltpu.SemaphoreType.DMA
    return pl.pallas_call(
        functools.partial(kernel, n_grp, n_dev, cols),
        out_shape=jax.ShapeDtypeStruct((rank, cols), jnp.float32),
        in_specs=[vmem, vmem, vmem, vmem, any_spec, any_spec, any_spec],
        out_specs=vmem,
        scratch_shapes=[
            VMEM((n_grp, n_dev, rows, LANES), jnp.bfloat16),
            VMEM((user_dev * n_dev, LANES), jnp.float32),
            VMEM((sub_dev, n_dev * rank), jnp.bfloat16),
            VMEM((2, width, LANES), jnp.float32),
            pltpu.SMEM((STEP, width), jnp.int32),
            pltpu.SMEM((STEP, width), jnp.int32),
            pltpu.SMEM(tile_word.shape, jnp.int32),
            pltpu.SMEM(word_owner.shape, jnp.int32),
            VMEM((tiles, LANES), jnp.float32),
            VMEM((n_all, CAP, LANES), jnp.float32),
            VMEM((n_all, CAP, LANES), jnp.float32),
            dma((2,)), dma((2,)), dma((pairs,)), dma((pairs,)), dma((n_grp, pairs)), dma((n_grp, pairs)),
            dma((n_grp, pairs)), dma((n_grp, pairs)), dma((n_all,)), dma((n_all,)),
        ],
        compiler_params=pltpu.CompilerParams(collective_id=0, has_side_effects=True,
                                             vmem_limit_bytes=63_000_000),
        name="mttkrp",
    )(uf, sf, nz_value, nz_sub, nz_user, tile_word, word_owner)


def solution(mesh):
    n_grp, n_dev = mesh.shape["grp"], mesh.shape["dev"]

    def shards(nz_user, nz_sub, nz_value, tile_word, word_owner, user_factor, sub_factor):
        return mttkrp(n_grp, n_dev, nz_user, nz_sub, nz_value, tile_word, word_owner,
                      user_factor, sub_factor)

    return jax.shard_map(
        shards,
        mesh=mesh,
        in_specs=(
            jax.sharding.PartitionSpec(("grp", "dev"), None),
            jax.sharding.PartitionSpec(("grp", "dev"), None),
            jax.sharding.PartitionSpec(("grp", "dev"), None),
            jax.sharding.PartitionSpec(("grp", "dev")),
            jax.sharding.PartitionSpec(),
            jax.sharding.PartitionSpec(None, "dev"),
            jax.sharding.PartitionSpec(None, "dev"),
        ),
        out_specs=jax.sharding.PartitionSpec(None, ("grp", "dev")),
        check_vma=False,
    )
```
